32 devices in a mesh: ga: 8 (over z, x), ta: 4 (over y, core).
Axes of the slice: x: 2, y: 2, z: 4, core: 2. Of those that a mesh axis runs over, the one named last changes fastest.
Arguments:
- density: bfloat16 [2, 6144, 16384], P(None, 'ga', 'ta'), may hold values from -6 to 6
- coulomb: float32 [6144], P('ga'), may hold values from 0.001275776 to 0.01275776
- row_block: int32 [1], replicated, may hold values from 0 to 67
Outputs:
- kernel: float32 [4, 4096, 2, 240], P('ta', 'ga')
The draws below stay inside these ranges and needn't reach their ends.
Inputs may be any that keep to these rules, and one draw needn't show every extreme that they name: The rows row_block * 240 to row_block * 240 + 239 lie among the 16384 transitions.
All inputs are finite; a program needn't handle non-finite values.
Results may differ from the reference program's by a relative error of at most 0.0025.
Values may be sent and summed in bfloat16 or wider, within the bound.
A program may use at most 64 MiB of HBM per device.

```python
import math
import jax
import jax.numpy as jnp
from jax import lax

NG = 6144
NC = 16384
RB = 240
N_TA = 4


def shard_levels(key, dims, shards, least, high):
    gain, own = 1.0, jax.random.fold_in(key, 6)
    for position, shards_of in shards:
        steps = jnp.exp(jax.random.uniform(jax.random.fold_in(own, position), (shards_of,), jnp.float32, least / len(shards), high / len(shards)))
        gain = gain * jnp.repeat(steps, dims[position] // shards_of).reshape([-1 if axis == position else 1 for axis in range(len(dims))])
    return gain


def gaussian(stream_key, shape, scale, most, split=(), held_as=jnp.bfloat16):
    drawn = jax.random.normal(stream_key, shape, jnp.float32) * scale
    if len(split) > 0:
        drawn = shard_levels(stream_key, shape, split, -0.22, 0.18) * drawn
    return jnp.clip(drawn, min=-most, max=most).astype(held_as)


def setup_inputs(seed: int = 0) -> dict:
    key_list = jax.random.split(jax.random.key(seed), 4)
    density = gaussian(key_list[0], (2, NG, NC), 1.0, 6.0, ((1, 8), (2, 4)))
    coulomb = jnp.clip(jnp.exp(math.log(0.01275776) - 2.3025851 * jax.random.uniform(key_list[1], (NG,), jnp.float32) ** shard_levels(key_list[1], (NG,), ((0, 8),), -0.2, 0.2)), 0.001275776, 0.01275776)
    row_block = jax.random.randint(key_list[2], (1,), 0, NC // RB).astype(jnp.int32)
    return dict(density=density, coulomb=coulomb, row_block=row_block)


def stack_left(folded):
    real_part = folded[0]
    imag_part = folded[1]
    upper_half = jnp.concatenate([real_part, -imag_part], axis=1)
    lower_half = jnp.concatenate([imag_part, real_part], axis=1)
    return jnp.concatenate([upper_half, lower_half], axis=0)


def reference(density, coulomb, row_block):
    offset = (row_block[0] * RB).astype(jnp.int32)
    picked = lax.dynamic_slice_in_dim(density, offset, RB, 2)
    folded = (coulomb[None, :, None] * picked.astype(jnp.float32)).astype(jnp.bfloat16)
    stacked = stack_left(folded)
    flattened = density.reshape(2 * NG, NC)
    kernel = lax.dot_general(flattened, stacked, (((0,), (0,)), ((), ())), preferred_element_type=jnp.float32)
    return kernel.reshape(N_TA, NC // N_TA, 2, RB)
```

```python
import functools

import jax
import jax.numpy as jnp
from jax import lax
from jax.experimental import pallas as pl
from jax.experimental.pallas import tpu as pltpu
from jax.sharding import PartitionSpec as P

RB = 240
LANES = 128
CHUNKS = (48, 48, 48, 48, 48)
ORDERS = ((0, 1, 2), (1, 0, 2), (0, 1, 2), (0, 1, 2), (0, 1, 2))
MESH = pl.DeviceIdType.MESH


def stack_left(folded):
    real_part = folded[0]
    imag_part = folded[1]
    upper_half = jnp.concatenate([real_part, -imag_part], axis=1)
    lower_half = jnp.concatenate([imag_part, real_part], axis=1)
    return jnp.concatenate([upper_half, lower_half], axis=0)


def plain_body(density, coulomb, row_block):
    local_g = density.shape[1]
    col_width = density.shape[2]
    group_index = lax.axis_index("ta")
    column = row_block[0] * RB + jnp.arange(RB, dtype=jnp.int32)
    owner_index = column // col_width
    position = jnp.clip(column - group_index * col_width, 0, col_width - 1)
    picked = jnp.take(density, position, axis=2)
    weighted = (coulomb[None, :, None] * picked.astype(jnp.float32)).astype(jnp.bfloat16)
    masked = jnp.where(
        (owner_index == group_index)[None, None, :], weighted.astype(jnp.float32), 0.0
    )
    folded = lax.psum(masked.astype(jnp.bfloat16), "ta")
    stacked = stack_left(folded)
    own_rows = col_width // lax.axis_size("ga")
    sliced = density.reshape(2 * local_g, lax.axis_size("ga") * own_rows)
    kernel = lax.psum_scatter(
        lax.dot_general(
            sliced, stacked, (((0,), (0,)), ((), ())), preferred_element_type=jnp.float32
        ),
        "ga",
        scatter_dimension=0,
        tiled=True,
    )
    return kernel.reshape(1, kernel.shape[0], 2, RB)


def pick_kernel(local_g, width, window, row_block, density, coulomb, out, held, sem):
    first = row_block[0] * RB - lax.axis_index("ta") * width
    start = jnp.minimum(lax.div(jnp.maximum(first, 0), LANES) * LANES, width - window)
    start = pl.multiple_of(start, LANES)
    copy = pltpu.make_async_copy(density.at[:, pl.ds(start, window)], held, sem)
    copy.start()
    row = lax.broadcasted_iota(jnp.int32, (RB, window), 0)
    column = lax.broadcasted_iota(jnp.int32, (RB, window), 1)
    chosen = jnp.where(start + column == first + row, 1.0, 0.0).astype(jnp.bfloat16)
    copy.wait()
    for part in range(2):
        picked = lax.dot_general(
            chosen,
            held[part * local_g : (part + 1) * local_g, :],
            (((1,), (1,)), ((), ())),
            preferred_element_type=jnp.float32,
        )
        out[part] = (coulomb[...] * picked).astype(jnp.bfloat16)


def flipped(index, bit):
    step = 2**bit
    return index + step * (1 - 2 * lax.rem(lax.div(index, step), 2))


def exchange_kernel(
    n_ga, local_g, own,
    masked, density, out,
    dens, half, other_half, far_half, full, lhs, acc, s0, r0, s1, r1, s2, r2,
    dens_sem, core_ss, core_rs, far_ss, far_rs, back_ss, back_rs,
    ss0, rs0, ss1, rs1, ss2, rs2,
):
    ga = lax.axis_index("ga")
    ta = lax.axis_index("ta")
    core = lax.rem(ta, 2)
    core_peer = {"ta": flipped(ta, 0)}
    far_peer = {"ta": flipped(ta, 1)}
    ga_peer = [{"ga": flipped(ga, bit)} for bit in range(3)]
    offsets = [sum(CHUNKS[:c]) for c in range(len(CHUNKS))]

    def block_of(relative_bits):
        index = ga
        for bit, flag in enumerate(relative_bits):
            step = 2**bit
            index = index + flag * step * (1 - 2 * lax.rem(lax.div(ga, step), 2))
        return index

    def load(r):
        bits = [lax.rem(lax.div(r, 2**bit), 2) for bit in range(3)]
        column = pl.multiple_of(block_of(bits) * own, own)
        return pltpu.make_async_copy(density.at[:, pl.ds(column, own)], dens.at[r], dens_sem.at[r])

    def start_load(i, carry):
        load(7 - i).start()
        return carry

    lax.fori_loop(0, n_ga, start_load, 0)

    barrier = pltpu.get_barrier_semaphore()
    peers = [core_peer, far_peer] + ga_peer
    for peer in peers:
        pl.semaphore_signal(barrier, inc=1, device_id=peer, device_id_type=MESH)
    pl.semaphore_wait(barrier, len(peers))

    def remote(src, dst, send, recv, peer):
        return pltpu.make_async_remote_copy(
            src_ref=src, dst_ref=dst, send_sem=send, recv_sem=recv,
            device_id=peer, device_id_type=MESH,
        )

    to_core = remote(masked.at[1 - core], other_half, core_ss, core_rs, core_peer)
    to_core.start()

    def to_far(c):
        rows = pl.ds(offsets[c], CHUNKS[c])
        return remote(half.at[rows], far_half.at[rows], far_ss.at[c], far_rs.at[c], far_peer)

    def back(c, part):
        rows = pl.ds(offsets[c], CHUNKS[c])
        view = full.at[part, rows]
        return remote(view, view, back_ss.at[c], back_rs.at[c], core_peer)

    to_core.wait_recv()
    f32 = jnp.float32
    for c, size in enumerate(CHUNKS):
        rows = pl.ds(offsets[c], size)
        half[rows] = (masked[core, rows].astype(f32) + other_half[rows].astype(f32)).astype(jnp.bfloat16)
        to_far(c).start()

    def prepare(c):
        rows = pl.ds(offsets[c], CHUNKS[c])
        to_far(c).wait_recv()
        full[core, rows] = (half[rows].astype(f32) + far_half[rows].astype(f32)).astype(jnp.bfloat16)
        back(c, core).start()

    def both(c):
        return pl.ds(2 * offsets[c], 2 * CHUNKS[c])

    def send0(c, q):
        view = both(c)
        sem = 4 * c + q
        return remote(s0.at[q, view], r0.at[q, view], ss0.at[sem], rs0.at[sem], ga_peer[ORDERS[c][0]])

    def send1(c, k):
        view = both(c)
        sem = 2 * c + k
        return remote(s1.at[k, view], r1.at[k, view], ss1.at[sem], rs1.at[sem], ga_peer[ORDERS[c][1]])

    def send2(c):
        view = both(c)
        return remote(s2.at[view], r2.at[view], ss2.at[c], rs2.at[c], ga_peer[ORDERS[c][2]])

    def base(c, q):
        _, second, third = ORDERS[c]
        return 2**second * (1 - lax.div(q, 2)) + 2**third * (1 - lax.rem(q, 2))

    def product(c, r):
        return jnp.dot(lhs[both(c)], dens[r], preferred_element_type=f32)

    def fill_left(c):
        rows = pl.ds(offsets[c], CHUNKS[c])
        back(c, 1 - core).wait_recv()
        real_part = full[0, rows]
        imag_part = full[1, rows]
        upper = pl.ds(2 * offsets[c], CHUNKS[c])
        lower = pl.ds(2 * offsets[c] + CHUNKS[c], CHUNKS[c])
        lhs[upper, 0:local_g] = real_part
        lhs[upper, local_g : 2 * local_g] = imag_part
        lhs[lower, 0:local_g] = -imag_part
        lhs[lower, local_g : 2 * local_g] = real_part

    def sent_products(c):
        def step(q, carry):
            r = base(c, q) + 2 ** ORDERS[c][0]
            if c == 0:
                load(r).wait()
            s0[q, both(c)] = product(c, r).astype(jnp.bfloat16)
            send0(c, q).start()
            return carry

        lax.fori_loop(0, 4, step, 0)

    def kept_products(c):
        def step(q, carry):
            r = base(c, q)
            if c == 0:
                load(r).wait()
            acc[q, both(c)] = product(c, r)
            return carry

        lax.fori_loop(0, 4, step, 0)

    def second_stage(c):
        view = both(c)
        for k in range(2):
            send0(c, k).wait_recv()
            s1[k, view] = (acc[k, view] + r0[k, view].astype(f32)).astype(jnp.bfloat16)
            send1(c, k).start()

    def third_stage(c):
        view = both(c)
        send0(c, 2).wait_recv()
        send1(c, 0).wait_recv()
        s2[view] = (acc[2, view] + r0[2, view].astype(f32) + r1[0, view].astype(f32)).astype(jnp.bfloat16)
        send2(c).start()

    def last_stage(c):
        send0(c, 3).wait_recv()
        send1(c, 1).wait_recv()
        send2(c).wait_recv()
        for part in range(2):
            view = pl.ds(2 * offsets[c] + part * CHUNKS[c], CHUNKS[c])
            out[part, pl.ds(offsets[c], CHUNKS[c])] = (
                acc[3, view] + r0[3, view].astype(f32) + r1[1, view].astype(f32) + r2[view].astype(f32)
            )

    count = len(CHUNKS)
    prepare(0)
    for c in range(count + 3):
        if c < count:
            fill_left(c)
            sent_products(c)
            if c + 1 < count:
                prepare(c + 1)
            kept_products(c)
        if 0 <= c - 1 < count:
            second_stage(c - 1)
        if 0 <= c - 2 < count:
            third_stage(c - 2)
        if 0 <= c - 3 < count:
            last_stage(c - 3)

    to_core.wait_send()
    for c in range(count):
        to_far(c).wait_send()
        back(c, core).wait_send()
        for q in range(4):
            send0(c, q).wait_send()
        for k in range(2):
            send1(c, k).wait_send()
        send2(c).wait_send()


def kernel_body(n_ga, density, coulomb, row_block):
    local_g = density.shape[1]
    width = density.shape[2]
    own = width // n_ga
    flat = density.reshape(2 * local_g, width)
    window = -(-(RB + LANES - 1) // LANES) * LANES
    bf16, f32 = jnp.bfloat16, jnp.float32
    vmem, anywhere = pl.BlockSpec(memory_space=pltpu.VMEM), pl.BlockSpec(memory_space=pl.ANY)
    masked = pl.pallas_call(
        functools.partial(pick_kernel, local_g, width, window),
        out_shape=jax.ShapeDtypeStruct((2, RB, local_g), bf16),
        in_specs=[pl.BlockSpec(memory_space=pltpu.SMEM), anywhere, vmem],
        out_specs=vmem,
        scratch_shapes=[pltpu.VMEM((2 * local_g, window), bf16), pltpu.SemaphoreType.DMA],
    )(row_block, flat, coulomb.reshape(1, local_g))
    count = len(CHUNKS)
    dma = pltpu.SemaphoreType.DMA
    kernel = pl.pallas_call(
        functools.partial(exchange_kernel, n_ga, local_g, own),
        out_shape=jax.ShapeDtypeStruct((2, RB, own), f32),
        in_specs=[vmem, anywhere],
        out_specs=vmem,
        scratch_shapes=[
            pltpu.VMEM((n_ga, 2 * local_g, own), bf16),
            pltpu.VMEM((RB, local_g), bf16),
            pltpu.VMEM((RB, local_g), bf16),
            pltpu.VMEM((RB, local_g), bf16),
            pltpu.VMEM((2, RB, local_g), bf16),
            pltpu.VMEM((2 * RB, 2 * local_g), bf16),
            pltpu.VMEM((4, 2 * RB, own), f32),
            pltpu.VMEM((4, 2 * RB, own), bf16),
            pltpu.VMEM((4, 2 * RB, own), bf16),
            pltpu.VMEM((2, 2 * RB, own), bf16),
            pltpu.VMEM((2, 2 * RB, own), bf16),
            pltpu.VMEM((2 * RB, own), bf16),
            pltpu.VMEM((2 * RB, own), bf16),
            dma((n_ga,)),
            dma, dma,
            dma((count,)), dma((count,)),
            dma((count,)), dma((count,)),
            dma((4 * count,)), dma((4 * count,)),
            dma((2 * count,)), dma((2 * count,)),
            dma((count,)), dma((count,)),
        ],
        compiler_params=pltpu.CompilerParams(collective_id=0, has_side_effects=True),
    )(masked, flat)
    return jnp.transpose(kernel, (2, 0, 1))[None]


def solution(mesh):
    in_specs = (P(None, "ga", "ta"), P("ga"), P())
    out_specs = P("ta", "ga", None, None)
    n_ga, n_ta = mesh.shape["ga"], mesh.shape["ta"]

    def body(density, coulomb, row_block):
        _, local_g, width = density.shape
        aligned = local_g % LANES == 0 and width % (n_ga * LANES) == 0
        if aligned and n_ga == 8 and n_ta == 4:
            return kernel_body(n_ga, density, coulomb, row_block)
        return plain_body(density, coulomb, row_block)

    return jax.shard_map(body, mesh=mesh, in_specs=in_specs, out_specs=out_specs, check_vma=False)
```

```python
import functools

import jax
import jax.numpy as jnp
from jax import lax
from jax.experimental import pallas as pl
from jax.experimental.pallas import tpu as pltpu
from jax.sharding import PartitionSpec as P

RB = 240
LANES = 128
CHUNKS = (48, 48, 48, 48, 48)
ORDERS = ((0, 1, 2), (1, 0, 2), (0, 1, 2), (0, 1, 2), (0, 1, 2))
MESH = pl.DeviceIdType.MESH
VMEM_BYTES = 56 * 2**20
PICK_BYTES = 56 * 2**20
LAGS = (1, 2, 3)


def stack_left(folded):
    real_part = folded[0]
    imag_part = folded[1]
    upper_half = jnp.concatenate([real_part, -imag_part], axis=1)
    lower_half = jnp.concatenate([imag_part, real_part], axis=1)
    return jnp.concatenate([upper_half, lower_half], axis=0)


def plain_body(density, coulomb, row_block):
    local_g = density.shape[1]
    col_width = density.shape[2]
    group_index = lax.axis_index("ta")
    column = row_block[0] * RB + jnp.arange(RB, dtype=jnp.int32)
    owner_index = column // col_width
    position = jnp.clip(column - group_index * col_width, 0, col_width - 1)
    picked = jnp.take(density, position, axis=2)
    weighted = (coulomb[None, :, None] * picked.astype(jnp.float32)).astype(jnp.bfloat16)
    masked = jnp.where(
        (owner_index == group_index)[None, None, :], weighted.astype(jnp.float32), 0.0
    )
    folded = lax.psum(masked.astype(jnp.bfloat16), "ta")
    stacked = stack_left(folded)
    own_rows = col_width // lax.axis_size("ga")
    sliced = density.reshape(2 * local_g, lax.axis_size("ga") * own_rows)
    kernel = lax.psum_scatter(
        lax.dot_general(
            sliced, stacked, (((0,), (0,)), ((), ())), preferred_element_type=jnp.float32
        ),
        "ga",
        scatter_dimension=0,
        tiled=True,
    )
    return kernel.reshape(1, kernel.shape[0], 2, RB)


def pick_kernel(local_g, width, window, row_block, density, coulomb, out, held, sem):
    first = row_block[0] * RB - lax.axis_index("ta") * width
    start = jnp.minimum(lax.div(jnp.maximum(first, 0), LANES) * LANES, width - window)
    start = pl.multiple_of(start, LANES)
    copy = pltpu.make_async_copy(density.at[:, pl.ds(start, window)], held, sem)
    copy.start()
    row = lax.broadcasted_iota(jnp.int32, (RB, window), 0)
    column = lax.broadcasted_iota(jnp.int32, (RB, window), 1)
    chosen = jnp.where(start + column == first + row, 1.0, 0.0).astype(jnp.bfloat16)
    copy.wait()
    for part in range(2):
        picked = lax.dot_general(
            chosen,
            held[part * local_g : (part + 1) * local_g, :],
            (((1,), (1,)), ((), ())),
            preferred_element_type=jnp.float32,
        )
        out[part] = (coulomb[...][None, :] * picked).astype(jnp.bfloat16)


def flipped(index, bit):
    step = 2**bit
    return index + step * (1 - 2 * lax.rem(lax.div(index, step), 2))


def exchange_kernel(
    n_ga, local_g, own,
    masked, density, out,
    dens, half, other_half, far_half, full, lhs, acc, s0, r0, s1, r1, s2, r2,
    dens_sem, core_ss, core_rs, far_ss, far_rs, back_ss, back_rs,
    ss0, rs0, ss1, rs1, ss2, rs2,
):
    ga = lax.axis_index("ga")
    ta = lax.axis_index("ta")
    core = lax.rem(ta, 2)
    core_peer = {"ta": flipped(ta, 0)}
    far_peer = {"ta": flipped(ta, 1)}
    ga_peer = [{"ga": flipped(ga, bit)} for bit in range(3)]
    offsets = [sum(CHUNKS[:c]) for c in range(len(CHUNKS))]

    def block_of(relative_bits):
        index = ga
        for bit, flag in enumerate(relative_bits):
            step = 2**bit
            index = index + flag * step * (1 - 2 * lax.rem(lax.div(ga, step), 2))
        return index

    def load(r):
        bits = [lax.rem(lax.div(r, 2**bit), 2) for bit in range(3)]
        column = pl.multiple_of(block_of(bits) * own, own)
        return pltpu.make_async_copy(density.at[:, pl.ds(column, own)], dens.at[r], dens_sem.at[r])

    def start_load(i, carry):
        load(7 - i).start()
        return carry

    lax.fori_loop(0, n_ga, start_load, 0)

    barrier = pltpu.get_barrier_semaphore()
    peers = [core_peer, far_peer] + ga_peer
    for peer in peers:
        pl.semaphore_signal(barrier, inc=1, device_id=peer, device_id_type=MESH)
    pl.semaphore_wait(barrier, len(peers))

    def remote(src, dst, send, recv, peer):
        return pltpu.make_async_remote_copy(
            src_ref=src, dst_ref=dst, send_sem=send, recv_sem=recv,
            device_id=peer, device_id_type=MESH,
        )

    def to_core(c):
        rows = pl.ds(offsets[c], CHUNKS[c])
        return remote(
            masked.at[1 - core, rows], other_half.at[rows], core_ss.at[c], core_rs.at[c], core_peer
        )

    for c in range(len(CHUNKS)):
        to_core(c).start()

    def to_far(c):
        rows = pl.ds(offsets[c], CHUNKS[c])
        return remote(half.at[rows], far_half.at[rows], far_ss.at[c], far_rs.at[c], far_peer)

    def back(c, part):
        rows = pl.ds(offsets[c], CHUNKS[c])
        view = full.at[part, rows]
        return remote(view, view, back_ss.at[c], back_rs.at[c], core_peer)

    f32 = jnp.float32
    for c, size in enumerate(CHUNKS):
        rows = pl.ds(offsets[c], size)
        to_core(c).wait_recv()
        half[rows] = (masked[core, rows].astype(f32) + other_half[rows].astype(f32)).astype(jnp.bfloat16)
        to_far(c).start()

    def prepare(c):
        rows = pl.ds(offsets[c], CHUNKS[c])
        to_far(c).wait_recv()
        full[core, rows] = (half[rows].astype(f32) + far_half[rows].astype(f32)).astype(jnp.bfloat16)
        back(c, core).start()

    def both(c):
        return pl.ds(2 * offsets[c], 2 * CHUNKS[c])

    def send0(c, q):
        view = both(c)
        sem = 4 * c + q
        return remote(s0.at[q, view], r0.at[q, view], ss0.at[sem], rs0.at[sem], ga_peer[ORDERS[c][0]])

    def send1(c, k):
        view = both(c)
        sem = 2 * c + k
        return remote(s1.at[k, view], r1.at[k, view], ss1.at[sem], rs1.at[sem], ga_peer[ORDERS[c][1]])

    def send2(c):
        view = both(c)
        return remote(s2.at[view], r2.at[view], ss2.at[c], rs2.at[c], ga_peer[ORDERS[c][2]])

    def base(c, q):
        _, second, third = ORDERS[c]
        return 2**second * (1 - lax.div(q, 2)) + 2**third * (1 - lax.rem(q, 2))

    def product(c, r):
        return jnp.dot(lhs[both(c)], dens[r], preferred_element_type=f32)

    def fill_left(c):
        rows = pl.ds(offsets[c], CHUNKS[c])
        back(c, 1 - core).wait_recv()
        real_part = full[0, rows]
        imag_part = full[1, rows]
        upper = pl.ds(2 * offsets[c], CHUNKS[c])
        lower = pl.ds(2 * offsets[c] + CHUNKS[c], CHUNKS[c])
        lhs[upper, 0:local_g] = real_part
        lhs[upper, local_g : 2 * local_g] = imag_part
        lhs[lower, 0:local_g] = -imag_part
        lhs[lower, local_g : 2 * local_g] = real_part

    def sent_products(c):
        def step(q, carry):
            r = base(c, q) + 2 ** ORDERS[c][0]
            if c == 0:
                load(r).wait()
            s0[q, both(c)] = product(c, r).astype(jnp.bfloat16)
            send0(c, q).start()
            return carry

        lax.fori_loop(0, 4, step, 0)

    def kept_products(c):
        def step(q, carry):
            r = base(c, q)
            if c == 0:
                load(r).wait()
            acc[q, both(c)] = product(c, r)
            return carry

        lax.fori_loop(0, 4, step, 0)

    def second_stage(c):
        view = both(c)
        for k in range(2):
            send0(c, k).wait_recv()
            s1[k, view] = (acc[k, view] + r0[k, view].astype(f32)).astype(jnp.bfloat16)
            send1(c, k).start()

    def third_stage(c):
        view = both(c)
        send0(c, 2).wait_recv()
        send1(c, 0).wait_recv()
        s2[view] = (acc[2, view] + r0[2, view].astype(f32) + r1[0, view].astype(f32)).astype(jnp.bfloat16)
        send2(c).start()

    def last_stage(c):
        send0(c, 3).wait_recv()
        send1(c, 1).wait_recv()
        send2(c).wait_recv()
        for part in range(2):
            view = pl.ds(2 * offsets[c] + part * CHUNKS[c], CHUNKS[c])
            out[part, pl.ds(offsets[c], CHUNKS[c])] = (
                acc[3, view] + r0[3, view].astype(f32) + r1[1, view].astype(f32) + r2[view].astype(f32)
            )

    count = len(CHUNKS)
    prepare(0)
    for c in range(count + LAGS[2]):
        if c < count:
            fill_left(c)
            sent_products(c)
            if c + 1 < count:
                prepare(c + 1)
            kept_products(c)
        if 0 <= c - LAGS[0] < count:
            second_stage(c - LAGS[0])
        if 0 <= c - LAGS[1] < count:
            third_stage(c - LAGS[1])
        if 0 <= c - LAGS[2] < count:
            last_stage(c - LAGS[2])

    for c in range(count):
        to_core(c).wait_send()
        to_far(c).wait_send()
        back(c, core).wait_send()
        for q in range(4):
            send0(c, q).wait_send()
        for k in range(2):
            send1(c, k).wait_send()
        send2(c).wait_send()


def kernel_body(n_ga, density, coulomb, row_block):
    local_g = density.shape[1]
    width = density.shape[2]
    own = width // n_ga
    flat = density.reshape(2 * local_g, width)
    window = -(-(RB + LANES - 1) // LANES) * LANES
    bf16, f32 = jnp.bfloat16, jnp.float32
    vmem, anywhere = pl.BlockSpec(memory_space=pltpu.VMEM), pl.BlockSpec(memory_space=pl.ANY)
    masked = pl.pallas_call(
        functools.partial(pick_kernel, local_g, width, window),
        out_shape=jax.ShapeDtypeStruct((2, RB, local_g), bf16),
        in_specs=[pl.BlockSpec(memory_space=pltpu.SMEM), anywhere, vmem],
        out_specs=vmem,
        scratch_shapes=[pltpu.VMEM((2 * local_g, window), bf16), pltpu.SemaphoreType.DMA],
        compiler_params=pltpu.CompilerParams(vmem_limit_bytes=PICK_BYTES),
    )(row_block, flat, coulomb)
    count = len(CHUNKS)
    dma = pltpu.SemaphoreType.DMA
    kernel = pl.pallas_call(
        functools.partial(exchange_kernel, n_ga, local_g, own),
        out_shape=jax.ShapeDtypeStruct((2, RB, own), f32),
        in_specs=[vmem, anywhere],
        out_specs=vmem,
        scratch_shapes=[
            pltpu.VMEM((n_ga, 2 * local_g, own), bf16),
            pltpu.VMEM((RB, local_g), bf16),
            pltpu.VMEM((RB, local_g), bf16),
            pltpu.VMEM((RB, local_g), bf16),
            pltpu.VMEM((2, RB, local_g), bf16),
            pltpu.VMEM((2 * RB, 2 * local_g), bf16),
            pltpu.VMEM((4, 2 * RB, own), f32),
            pltpu.VMEM((4, 2 * RB, own), bf16),
            pltpu.VMEM((4, 2 * RB, own), bf16),
            pltpu.VMEM((2, 2 * RB, own), bf16),
            pltpu.VMEM((2, 2 * RB, own), bf16),
            pltpu.VMEM((2 * RB, own), bf16),
            pltpu.VMEM((2 * RB, own), bf16),
            dma((n_ga,)),
            dma((count,)), dma((count,)),
            dma((count,)), dma((count,)),
            dma((count,)), dma((count,)),
            dma((4 * count,)), dma((4 * count,)),
            dma((2 * count,)), dma((2 * count,)),
            dma((count,)), dma((count,)),
        ],
        compiler_params=pltpu.CompilerParams(
            collective_id=0, has_side_effects=True, vmem_limit_bytes=VMEM_BYTES
        ),
    )(masked, flat)
    return jnp.transpose(kernel, (2, 0, 1))[None]


def solution(mesh):
    in_specs = (P(None, "ga", "ta"), P("ga"), P())
    out_specs = P("ta", "ga", None, None)
    n_ga, n_ta = mesh.shape["ga"], mesh.shape["ta"]

    def body(density, coulomb, row_block):
        _, local_g, width = density.shape
        aligned = local_g % LANES == 0 and width % (n_ga * LANES) == 0
        if aligned and n_ga == 8 and n_ta == 4:
            return kernel_body(n_ga, density, coulomb, row_block)
        return plain_body(density, coulomb, row_block)

    return jax.shard_map(body, mesh=mesh, in_specs=in_specs, out_specs=out_specs, check_vma=False)
```
